32 devices in a mesh: rep: 4 (over x, y), dp: 8 (over z, core).
Axes of the slice: x: 2, y: 2, z: 4, core: 2. Of those that a mesh axis runs over, the one named last changes fastest.
Arguments:
- x: bfloat16 [32, 4096, 768], P(('rep', 'dp')), parts along dimension 0
- dy: bfloat16 [32, 4096, 768], P(('rep', 'dp')), parts along dimension 0
- w_gate: bfloat16 [2, 768, 1792], P(None, 'dp')
- w_up: bfloat16 [2, 768, 1792], P(None, 'dp')
- w_down: bfloat16 [2, 1792, 768], P(None, 'dp')
- m_w_gate: float32 [2, 768, 1792], P(None, 'dp')
- m_w_up: float32 [2, 768, 1792], P(None, 'dp')
- m_w_down: float32 [2, 1792, 768], P(None, 'dp')
- v_w_gate: float32 [2, 768, 1792], P(None, 'dp')
- v_w_up: float32 [2, 768, 1792], P(None, 'dp')
- v_w_down: float32 [2, 1792, 768], P(None, 'dp')
Outputs:
- output 1: bfloat16 [8, 768, 1792], P('rep', 'dp'), parts along dimension 0
- output 2: bfloat16 [8, 768, 1792], P('rep', 'dp'), parts along dimension 0
- output 3: bfloat16 [8, 1792, 768], P('rep', 'dp'), parts along dimension 0
- output 4: float32 [8, 768, 1792], P('rep', 'dp'), parts along dimension 0
- output 5: float32 [8, 768, 1792], P('rep', 'dp'), parts along dimension 0
- output 6: float32 [8, 1792, 768], P('rep', 'dp'), parts along dimension 0
- output 7: float32 [8, 768, 1792], P('rep', 'dp'), parts along dimension 0
- output 8: float32 [8, 768, 1792], P('rep', 'dp'), parts along dimension 0
- output 9: float32 [8, 1792, 768], P('rep', 'dp'), parts along dimension 0
There are 4 independent parts. The reference program is written for one: setup_inputs(seed, part) draws one part's arguments, and reference() takes and returns one part's arrays. A program takes and returns all parts, laid end to end along the dimension named above; an argument that names none is the same for every part.
All inputs are finite; a program needn't handle non-finite values.
Results may differ from the reference program's by a relative error of at most 0.022.
Values are sent between devices in bfloat16 or wider.
A program may use at most 2 GiB of HBM per device.

```python
import jax
import jax.numpy as jnp
from jax import lax

SEQUENCES = 8
TOKENS = 4096
D = 768
FF = 1792
LAYERS = 2
NAMES = ("w_gate", "w_up", "w_down")
SHAPES = {"w_gate": (LAYERS, D, FF), "w_up": (LAYERS, D, FF), "w_down": (LAYERS, FF, D)}


def bump(key, n, height):
    away = (jnp.arange(n, dtype=jnp.int32) - jax.random.randint(key, (), 0, n, jnp.int32)) % n
    return jnp.where(away < n // 8, height, 1.0)


def together(key, own, strength):
    shared = jax.random.normal(key, own.shape[1:], jnp.float32)
    return (own + strength * shared) * lax.rsqrt(1 + strength * strength)


def setup_inputs(seed: int = 0, part: int = 0) -> dict:
    kx, kdy, ka, kb, kz, kf, kh, kl, *keys = jax.random.split(jax.random.key(seed), 8 + 3 * len(NAMES))
    kx, kdy, ka, kb = (jax.random.fold_in(k, part) for k in (kx, kdy, ka, kb))
    kw, km, kv = (keys[i::3] for i in range(3))
    shape = (SEQUENCES, TOKENS, D)
    much_x, much_dy = jax.random.uniform(kz, (2,), jnp.float32, 0.0, 1.0)
    loud = 2.0 ** jax.random.uniform(jax.random.fold_in(kz, 1), (), jnp.float32, -1.0, 2.0)
    layers = 2.0 ** jax.random.uniform(kl, (LAYERS, 1, 1), jnp.float32, -1.0, 1.0)
    x = together(ka, jax.random.normal(kx, shape, jnp.float32), much_x) * bump(kf, D, 4.0)
    dy = together(kb, jax.random.normal(kdy, shape, jnp.float32), much_dy)
    drawn = {"x": x.astype(jnp.bfloat16), "dy": (loud * dy * (SEQUENCES * TOKENS) ** -0.5).astype(jnp.bfloat16)}
    for key, name in zip(kw, NAMES, strict=True):
        w = jax.random.normal(key, SHAPES[name], jnp.float32) * SHAPES[name][1] ** -0.5
        drawn[name] = (w * {"w_gate": 1.0, "w_up": bump(kh, FF, 4.0), "w_down": layers}[name]).astype(jnp.bfloat16)
    for key, name in zip(km, NAMES, strict=True):
        drawn[f"m_{name}"] = 0.1 * jax.random.normal(key, SHAPES[name], jnp.float32)
    for key, name in zip(kv, NAMES, strict=True):
        drawn[f"v_{name}"] = jax.random.uniform(key, SHAPES[name], jnp.float32, 0.005, 0.015)
    return drawn


def matmul(a, w):
    return jnp.dot(a, w, preferred_element_type=jnp.float32).astype(jnp.bfloat16)


def normed(h):
    wide = h.astype(jnp.float32)
    scale = lax.rsqrt(jnp.mean(wide**2, -1, keepdims=True) + 1e-6)
    return (wide * scale).astype(jnp.bfloat16)


def layer(h, w):
    a = normed(h)
    gate = jnp.dot(a, w["w_gate"], preferred_element_type=jnp.float32)
    up = jnp.dot(a, w["w_up"], preferred_element_type=jnp.float32)
    return h + matmul((jax.nn.silu(gate) * up).astype(jnp.bfloat16), w["w_down"])


def adamw(w, m, v, g):
    m = 0.9 * m + 0.1 * g
    v = 0.95 * v + 0.05 * g * g
    step = m * lax.rsqrt(v + 1e-8) + 0.1 * w
    return (w - 0.02 * step).astype(jnp.bfloat16), m, v


def clipped(gradients, sum_of_squares, count):
    factor = jnp.minimum(1.0, 0.5 * lax.rsqrt(sum_of_squares / count + 1e-30))
    return [g * factor for g in gradients]


def stack(weights, h):
    return lax.scan(lambda h, w: (layer(h, w), None), h, weights)[0]


def reference(x, dy, w_gate, w_up, w_down, m_w_gate, m_w_up, m_w_down, v_w_gate, v_w_up, v_w_down):
    weights = dict(zip(NAMES, (w_gate, w_up, w_down), strict=True))

    def take(so_far, sequence):
        h, by_y = sequence
        _, back = jax.vjp(lambda w: stack(w, h), weights)
        return jax.tree.map(lambda total, term: total + term.astype(jnp.float32), so_far, back(by_y)[0]), None

    none_yet = {name: jnp.zeros(w.shape, jnp.float32) for name, w in weights.items()}
    by_weights, _ = lax.scan(take, none_yet, (x, dy))
    gradients = [by_weights[name].astype(jnp.bfloat16).astype(jnp.float32) for name in NAMES]
    gradients = clipped(gradients, sum(jnp.sum(g * g) for g in gradients), sum(g.size for g in gradients))
    new = [
        adamw(w.astype(jnp.float32), m, v, g)
        for w, m, v, g in zip((w_gate, w_up, w_down), (m_w_gate, m_w_up, m_w_down), (v_w_gate, v_w_up, v_w_down), gradients, strict=True)
    ]
    return tuple(one[which] for which in range(3) for one in new)
```

```python
import functools

import jax
import jax.numpy as jnp
from jax import lax
from jax.experimental import pallas as pl
from jax.experimental.pallas import tpu as pltpu
from jax.sharding import PartitionSpec as P

LAYERS, TOKENS, D, FF = 2, 4096, 768, 1792
REPS, LINE, CORES = 4, 4, 2
GROUP = LINE * CORES
CHUNK = 256
CHUNKS = FF // CHUNK
LOCAL = CHUNK // GROUP
ROWS = D // GROUP
HALF = ROWS // 2
TILE = 512
TILES = TOKENS // TILE
ALL = LAYERS * CHUNKS
F32, BF16 = jnp.float32, jnp.bfloat16


def adamw(w, m, v, g):
    m = 0.9 * m + 0.1 * g
    v = 0.95 * v + 0.05 * g * g
    step = m * lax.rsqrt(v + 1e-8) + 0.1 * w
    return (w - 0.02 * step).astype(BF16), m, v


def dot(a, b, ca=1, cb=0):
    return lax.dot_general(a, b, (((ca,), (cb,)), ((), ())), preferred_element_type=F32)


def norm_scale(wide):
    return lax.rsqrt(jnp.mean(wide * wide, -1, keepdims=True) + 1e-6)


def kernel(
    x_hbm, dy_hbm, gu_hbm, d_hbm, ggu_out, gd_out, ss_out,
    abuf, xb, dyb, acc, wgu, wd, gg, gd,
    s1gu, s1d, r1gu, r1d, own_gu, own_d, sum_gu, sum_d, s2gu, s2d, r2gu, r2d, ssb,
    xsem, dysem, ownsem, a1send, a1recv, a2send, a2recv, a3send, a3recv,
    c1send, c1recv, c2send, c2recv, sssend, ssrecv,
):
    rep, me = lax.axis_index("rep"), lax.axis_index("dp")
    z, k = me // CORES, me % CORES
    other = 1 - k
    rg, rh = rep // 2, rep % 2

    barrier = pltpu.get_barrier_semaphore()
    for o in range(1, GROUP):
        pl.semaphore_signal(barrier, 1, device_id={"dp": (me + o) % GROUP})
    for o in range(1, REPS):
        pl.semaphore_signal(barrier, 1, device_id={"rep": (rep + o) % REPS})

    def tokens(t):
        return pl.ds(pl.multiple_of(t * TILE, TILE), TILE)

    def fetch(hbm, vmem, sem, t):
        return pltpu.make_async_copy(hbm.at[0, tokens(t)], vmem.at[tokens(t)], sem.at[t])

    for t in range(TILES):
        fetch(x_hbm, xb, xsem, t).start()
        fetch(dy_hbm, dyb, dysem, t).start()
    pl.semaphore_wait(barrier, GROUP - 1 + REPS - 1)

    def quarter(i):
        layer, c = i // CHUNKS, i % CHUNKS
        columns = pl.ds(pl.multiple_of(c * CHUNK, CHUNK), CHUNK)
        return (
            gu_hbm.at[layer, rg, rh, :, columns],
            d_hbm.at[layer, c, rg, :, pl.ds(pl.multiple_of(rh * (D // 2), D // 2), D // 2)],
        )

    def half_d(i):
        return wd.at[i, :, k, rg, :, pl.ds(pl.multiple_of(rh * (D // 2), D // 2), D // 2)]

    def gather1(i):
        gu, down = quarter(i)
        gu_to = wgu.at[i, rg, z, k, rh]
        d_to = wd.at[i, z, k, rg, :, pl.ds(pl.multiple_of(rh * (D // 2), D // 2), D // 2)]
        for o in range(1, LINE):
            to = {"dp": (z + o) % LINE * CORES + k}
            pltpu.make_async_remote_copy(gu, gu_to, a1send.at[0], a1recv.at[0, i], device_id=to).start()
            pltpu.make_async_remote_copy(down, d_to, a1send.at[1], a1recv.at[1, i], device_id=to).start()
        pltpu.make_async_copy(gu, gu_to, ownsem.at[0, i]).start()
        pltpu.make_async_copy(down, d_to, ownsem.at[1, i]).start()

    def wait_bytes(ref, sem):
        pltpu.make_async_copy(ref, ref, sem).wait()

    def gather2(i):
        wait_bytes(wgu.at[i, 0, pl.ds(0, LINE - 1), 0, 0], a1recv.at[0, i])
        wait_bytes(wd.at[i, pl.ds(0, LINE - 1), 0, 0, :, pl.ds(0, D // 2)], a1recv.at[1, i])
        wait_bytes(wgu.at[i, 0, 0, 0, 0], ownsem.at[0, i])
        wait_bytes(wd.at[i, 0, 0, 0, :, pl.ds(0, D // 2)], ownsem.at[1, i])
        gu, down = wgu.at[i, rg, :, k, rh], half_d(i)
        for o in range(1, REPS):
            to = {"rep": (rep + o) % REPS}
            pltpu.make_async_remote_copy(gu, gu, a2send.at[0], a2recv.at[0, i], device_id=to).start()
            pltpu.make_async_remote_copy(down, down, a2send.at[1], a2recv.at[1, i], device_id=to).start()

    def gather3(i):
        wait_bytes(wgu.at[i, 0, pl.ds(0, REPS - 1)], a2recv.at[0, i])
        wait_bytes(wd.at[i, pl.ds(0, REPS - 1), :, 0], a2recv.at[1, i])
        gu, down = wgu.at[i, :, :, k], wd.at[i, :, k]
        to = {"dp": z * CORES + other}
        pltpu.make_async_remote_copy(gu, gu, a3send.at[0], a3recv.at[0, i], device_id=to).start()
        pltpu.make_async_remote_copy(down, down, a3send.at[1], a3recv.at[1, i], device_id=to).start()

    def arrived(i):
        wait_bytes(wgu.at[i, :, :, 0], a3recv.at[0, i])
        wait_bytes(wd.at[i, :, 0], a3recv.at[1, i])

    def gathered(i):
        pl.when(i + 2 < ALL)(lambda: gather2(i + 2))
        pl.when(i + 1 < ALL)(lambda: gather3(i + 1))
        arrived(i)

    pl.loop(0, ALL)(gather1)
    acc[...] = jnp.zeros_like(acc)

    @pl.loop(0, TILES)
    def _(t):
        fetch(x_hbm, xb, xsem, t).wait()
        wide = xb[tokens(t)].astype(F32)
        abuf[tokens(t)] = (wide * norm_scale(wide)).astype(BF16)

    gather2(0)
    gather2(1)
    gather3(0)

    def weights(i):
        gu = wgu[i]
        return gu[0].reshape(D, CHUNK), gu[1].reshape(D, CHUNK), wd[i].reshape(CHUNK, D)

    @pl.loop(0, CHUNKS)
    def _(c):
        gathered(c)

        @pl.loop(0, TILES)
        def _(t):
            wg, wu, down = weights(c)
            a = abuf[tokens(t)]
            gate, up = dot(a, wg), dot(a, wu)
            hidden = (gate * jax.nn.sigmoid(gate) * up).astype(BF16)
            acc[tokens(t)] += dot(hidden, down)

    @pl.loop(0, TILES)
    def _(t):
        h = xb[tokens(t)] + acc[tokens(t)].astype(BF16)
        xb[tokens(t)] = h
        wide = h.astype(F32)
        abuf[tokens(t)] = (wide * norm_scale(wide)).astype(BF16)
        acc[tokens(t)] = jnp.zeros((TILE, D), F32)
        fetch(dy_hbm, dyb, dysem, t).wait()

    def backward(i, t, first, with_input):
        wg, wu, down = weights(i)
        a, by_y = abuf[tokens(t)], dyb[tokens(t)]
        gate, up = dot(a, wg), dot(a, wu)
        by_hidden = dot(by_y, down, 1, 1).astype(BF16).astype(F32)
        s = jax.nn.sigmoid(gate)
        silu = gate * s
        hidden = (silu * up).astype(BF16)
        by_up = (by_hidden * silu).astype(BF16)
        by_gate = (by_hidden * up * (s + silu * (1.0 - s))).astype(BF16)

        def add(ref, value):
            ref[...] = value.reshape(ref.shape) if first else ref[...] + value.reshape(ref.shape)

        add(gd, dot(hidden, by_y, 0, 0))
        add(gg.at[0], dot(a, by_gate, 0, 0))
        add(gg.at[1], dot(a, by_up, 0, 0))
        if with_input:
            acc[tokens(t)] += dot(by_gate, wg, 1, 1) + dot(by_up, wu, 1, 1)

    def partner_copies(q):
        to, s = {"dp": z * CORES + other}, q % 2
        return (
            pltpu.make_async_remote_copy(s1gu, r1gu.at[s], c1send.at[0], c1recv.at[0, s], device_id=to),
            pltpu.make_async_remote_copy(s1d, r1d.at[s], c1send.at[1], c1recv.at[1, s], device_id=to),
        )

    def scatter1(q):
        s1gu[...] = gg[:, :, other].astype(BF16)
        s1d[...] = gd[:, other].astype(BF16)
        for copy in partner_copies(q):
            copy.start()
        own_gu[...] = gg[:, :, k]
        own_d[...] = gd[:, k]

    def wait_line_sends(s):
        wait_bytes(s2gu.at[s, pl.ds(0, LINE - 1)], c2send.at[0, s])
        wait_bytes(s2d.at[s, pl.ds(0, LINE - 1)], c2send.at[1, s])

    def scatter2(q):
        s = q % 2
        for copy in partner_copies(q):
            copy.wait()
        pl.when(q >= 2)(lambda: wait_line_sends(s))
        pair_gu = own_gu[...] + r1gu[s].astype(F32)
        pair_d = own_d[...] + r1d[s].astype(F32)
        for g in range(2):
            s2gu[s, :, g] = pair_gu[g].astype(BF16)
        s2d[s] = pair_d.astype(BF16)
        own_gu[...] = pair_gu
        own_d[...] = pair_d
        sum_gu[s] = own_gu[:, z]
        sum_d[s] = own_d[z]
        for o in range(1, LINE):
            there = (z + o) % LINE
            to = {"dp": there * CORES + k}
            pltpu.make_async_remote_copy(s2gu.at[s, there], r2gu.at[s, o - 1], c2send.at[0, s], c2recv.at[0, s, o - 1], device_id=to).start()
            pltpu.make_async_remote_copy(s2d.at[s, there], r2d.at[s, o - 1], c2send.at[1, s], c2recv.at[1, s, o - 1], device_id=to).start()

    def scatter3(q):
        s = q % 2
        for o in range(LINE - 1):
            wait_bytes(r2gu.at[s, o], c2recv.at[0, s, o])
            wait_bytes(r2d.at[s, o], c2recv.at[1, s, o])
        total_gu, total_d = sum_gu[s], sum_d[s]
        for o in range(LINE - 1):
            total_gu += r2gu[s, o].astype(F32)
            total_d += r2d[s, o].astype(F32)
        total_gu, total_d = total_gu.astype(BF16), total_d.astype(BF16)
        layer, c = LAYERS - 1 - q // CHUNKS, q % CHUNKS
        for g in range(2):
            ggu_out[layer, g, :, pl.ds(pl.multiple_of(c * CHUNK, CHUNK), CHUNK)] = total_gu[g]
        gd_out[layer, c] = total_d
        wide_gu, wide_d = total_gu.astype(F32), total_d.astype(F32)
        squares = (wide_gu * wide_gu).reshape(2, ROWS // 8, 8, CHUNK).sum((0, 1))
        squares_d = (wide_d * wide_d).reshape(LOCAL // 8, 8, D).sum(0)
        ssb[0] += sum(squares[:, n : n + 128] for n in range(0, CHUNK, 128)) + sum(squares_d[:, n : n + 128] for n in range(0, D, 128))

    ssb[0] = jnp.zeros((8, 128), F32)

    def layer_backward(base, q0, with_input, weights_come):
        @pl.loop(0, CHUNKS)
        def _(c):
            i, q = base + c, q0 + c
            if weights_come:
                gathered(i)
            backward(i, 0, True, with_input)
            pl.when(q >= 2)(lambda: scatter3(q - 2))
            pl.when(q >= 1)(lambda: scatter2(q - 1))

            @pl.loop(1, TILES)
            def _(t):
                backward(i, t, False, with_input)

            scatter1(q)

    layer_backward(CHUNKS, 0, True, True)

    @pl.loop(0, TILES)
    def _(t):
        wide = xb[tokens(t)].astype(F32)
        by_a = acc[tokens(t)].astype(BF16).astype(F32)
        scale = norm_scale(wide)
        inner = jnp.mean(wide * by_a, -1, keepdims=True)
        by_h = by_a * scale - wide * (scale * scale * scale * inner)
        dyb[tokens(t)] = dyb[tokens(t)] + by_h.astype(BF16)
        fetch(x_hbm, xb, xsem, t).start()

    @pl.loop(0, TILES)
    def _(t):
        fetch(x_hbm, xb, xsem, t).wait()
        wide = xb[tokens(t)].astype(F32)
        abuf[tokens(t)] = (wide * norm_scale(wide)).astype(BF16)

    layer_backward(0, CHUNKS, False, False)
    scatter3(ALL - 2)
    scatter2(ALL - 1)
    scatter3(ALL - 1)

    def square_copy(o):
        return pltpu.make_async_remote_copy(ssb.at[0], ssb.at[o], sssend.at[o - 1], ssrecv.at[o - 1], device_id={"dp": (me + o) % GROUP})

    for o in range(1, GROUP):
        square_copy(o).start()
    for o in range(1, GROUP):
        square_copy(o).wait()
    ss_out[...] = sum(ssb[o] for o in range(GROUP))

    for s in range(2):
        wait_line_sends(s)
    wait_bytes(wgu.at[:, 0, pl.ds(0, LINE - 1), 0, 0], a1send.at[0])
    wait_bytes(wd.at[:, pl.ds(0, LINE - 1), 0, 0, :, pl.ds(0, D // 2)], a1send.at[1])
    wait_bytes(wgu.at[:, 0, pl.ds(0, REPS - 1)], a2send.at[0])
    wait_bytes(wd.at[:, pl.ds(0, REPS - 1), :, 0], a2send.at[1])
    wait_bytes(wgu.at[:, :, :, 0], a3send.at[0])
    wait_bytes(wd.at[:, :, 0], a3send.at[1])


def gradients(x, dy, gu, down):
    vm, dma = pltpu.VMEM, pltpu.SemaphoreType.DMA
    flops = 17 * 2 * TOKENS * D * FF
    return pl.pallas_call(
        kernel,
        out_shape=(
            jax.ShapeDtypeStruct((LAYERS, 2, ROWS, FF), BF16),
            jax.ShapeDtypeStruct((LAYERS, CHUNKS, LOCAL, D), BF16),
            jax.ShapeDtypeStruct((8, 128), F32),
        ),
        in_specs=[pl.BlockSpec(memory_space=pl.ANY)] * 4,
        out_specs=(pl.BlockSpec(memory_space=pltpu.VMEM),) * 3,
        scratch_shapes=[
            vm((TOKENS, D), BF16), vm((TOKENS, D), BF16), vm((TOKENS, D), BF16), vm((TOKENS, D), F32),
            vm((ALL, 2, LINE, CORES, 2, HALF, CHUNK), BF16), vm((ALL, LINE, CORES, 2, LOCAL // 2, D), BF16),
            vm((2, LINE, CORES, ROWS, CHUNK), F32), vm((LINE, CORES, LOCAL, D), F32),
            vm((2, LINE, ROWS, CHUNK), BF16), vm((LINE, LOCAL, D), BF16),
            vm((2, 2, LINE, ROWS, CHUNK), BF16), vm((2, LINE, LOCAL, D), BF16),
            vm((2, LINE, ROWS, CHUNK), F32), vm((LINE, LOCAL, D), F32),
            vm((2, 2, ROWS, CHUNK), F32), vm((2, LOCAL, D), F32),
            vm((2, LINE, 2, ROWS, CHUNK), BF16), vm((2, LINE, LOCAL, D), BF16),
            vm((2, LINE - 1, 2, ROWS, CHUNK), BF16), vm((2, LINE - 1, LOCAL, D), BF16),
            vm((GROUP, 8, 128), F32),
            dma((TILES,)), dma((TILES,)), dma((2, ALL)), dma((2,)), dma((2, ALL)), dma((2,)), dma((2, ALL)), dma((2,)), dma((2, ALL)),
            dma((2,)), dma((2, 2)), dma((2, 2)), dma((2, 2, LINE - 1)), dma((GROUP - 1,)), dma((GROUP - 1,)),
        ],
        compiler_params=pltpu.CompilerParams(collective_id=0, has_side_effects=True, vmem_limit_bytes=67043328),
        cost_estimate=pl.CostEstimate(flops=flops, bytes_accessed=2 * TOKENS * D * 2, transcendentals=0),
    )(x, dy, gu, down)


def solution(mesh):
    def step(x, dy, w_gate, w_up, w_down, m_gate, m_up, m_down, v_gate, v_up, v_down):
        at = lax.broadcasted_iota(jnp.int32, (FF, FF), 0)
        to = lax.broadcasted_iota(jnp.int32, (FF, FF), 1)
        own = (to % CHUNK) // LOCAL * (FF // GROUP) + to // CHUNK * LOCAL + to % LOCAL
        order = (at == own).astype(BF16)
        gu = jnp.stack([w_gate, w_up], 1)
        placed = jnp.dot(gu.reshape(-1, FF), order, preferred_element_type=F32).astype(BF16)
        ggu, gd, squares = gradients(
            x, dy, placed.reshape(LAYERS, 2, 2, HALF, FF), w_down.reshape(LAYERS, CHUNKS, 2, LOCAL // 2, D)
        )
        ggu = lax.dot_general(ggu.reshape(-1, FF), order, (((1,), (1,)), ((), ())), preferred_element_type=F32).reshape(LAYERS, 2, ROWS, FF)
        g = [ggu[:, 0], ggu[:, 1], gd.reshape(w_down.shape).astype(F32)]
        count = GROUP * sum(one.size for one in g)
        factor = jnp.minimum(1.0, 0.5 * lax.rsqrt(jnp.sum(squares) / count + 1e-30))
        new = [
            adamw(w.astype(F32), m, v, one * factor)
            for w, m, v, one in zip((w_gate, w_up, w_down), (m_gate, m_up, m_down), (v_gate, v_up, v_down), g, strict=True)
        ]
        return tuple(one[which] for which in range(3) for one in new)

    states, cut = P(("rep", "dp"), None, None), P(None, "dp", None)
    return jax.shard_map(
        step,
        mesh=mesh,
        in_specs=(states, states) + (cut,) * 9,
        out_specs=(P("rep", "dp", None),) * 9,
        check_vma=False,
    )
```

```python
import functools

import jax
import jax.numpy as jnp
import numpy as np
from jax import lax
from jax.experimental import pallas as pl
from jax.experimental.pallas import tpu as pltpu
from jax.sharding import PartitionSpec as P

LAYERS, TOKENS, D, FF = 2, 4096, 768, 1792
REPS, LINE, CORES = 4, 4, 2
GROUP = LINE * CORES
CHUNK = 256
CHUNKS = FF // CHUNK
LOCAL = CHUNK // GROUP
ROWS = D // GROUP
HALF = ROWS // 2
TILE = 1024
TILES = TOKENS // TILE
AHEAD = 4
SLOTS = 3
ALL = LAYERS * CHUNKS
F32, BF16 = jnp.float32, jnp.bfloat16
ORDER = np.arange(FF, dtype=np.int32).reshape(GROUP, CHUNKS, LOCAL).transpose(1, 0, 2).reshape(FF)


def adamw(w, m, v, g):
    m = 0.9 * m + 0.1 * g
    v = 0.95 * v + 0.05 * g * g
    step = m * lax.rsqrt(v + 1e-8) + 0.1 * w
    return (w - 0.02 * step).astype(BF16), m, v


def dot(a, b, ca=1, cb=0):
    return lax.dot_general(a, b, (((ca,), (cb,)), ((), ())), preferred_element_type=F32)


def norm_scale(wide):
    return lax.rsqrt(jnp.mean(wide * wide, -1, keepdims=True) + 1e-6)


def kernel(
    x_hbm, dy_hbm, gu_hbm, d_hbm, ggu_out, gd_out, ss_out,
    abuf, xb, dyb, acc, wgu, wd, gg, gd,
    s1gu, s1d, r1gu, r1d, sum_gu, sum_d, s2gu, s2d, r2gu, r2d, sogu, sod, rogu, rod, sumogu, sumod, s3gu, s3d, r3gu, r3d, ssb,
    xsem, dysem, ownsem, a1send, a1recv, a2send, a2recv, a3send, a3recv,
    c1send, c1recv, c2send, c2recv, cosend, corecv, c3send, c3recv, mate_free, across_free, sssend, ssrecv,
):
    rep, me = lax.axis_index("rep"), lax.axis_index("dp")
    z, k = me // CORES, me % CORES
    other = 1 - k
    rg, rh = rep // 2, rep % 2

    barrier = pltpu.get_barrier_semaphore()
    for o in range(1, GROUP):
        pl.semaphore_signal(barrier, 1, device_id={"dp": (me + o) % GROUP})
    for o in range(1, REPS):
        pl.semaphore_signal(barrier, 1, device_id={"rep": (rep + o) % REPS})

    def tokens(t):
        return pl.ds(pl.multiple_of(t * TILE, TILE), TILE)

    def fetch(hbm, vmem, sem, t):
        return pltpu.make_async_copy(hbm.at[0, tokens(t)], vmem.at[tokens(t)], sem.at[t])

    for t in range(TILES):
        fetch(x_hbm, xb, xsem, t).start()
        fetch(dy_hbm, dyb, dysem, t).start()
    pl.semaphore_wait(barrier, GROUP - 1 + REPS - 1)

    def wait_bytes(ref, sem):
        pltpu.make_async_copy(ref, ref, sem).wait()

    d_half = pl.ds(pl.multiple_of(rh * (D // 2), D // 2), D // 2)

    def quarter(i, line):
        return wgu.at[i, rg, line, k, rh], wd.at[i, line, k, rg, :, d_half]

    def gather1(i):
        layer, c = i // CHUNKS, i % CHUNKS
        columns = pl.ds(pl.multiple_of(c * CHUNK, CHUNK), CHUNK)
        gu, down = gu_hbm.at[layer, rg, rh, :, columns], d_hbm.at[layer, c, rg, :, d_half]
        gu_to, d_to = quarter(i, z)
        for o in range(1, LINE):
            to = {"dp": (z + o) % LINE * CORES + k}
            pltpu.make_async_remote_copy(gu, gu_to, a1send.at[0], a1recv.at[0, i], device_id=to).start()
            pltpu.make_async_remote_copy(down, d_to, a1send.at[1], a1recv.at[1, i], device_id=to).start()
        pltpu.make_async_copy(gu_hbm.at[layer, :, :, :, columns], wgu.at[i, :, z, k], ownsem.at[0, i]).start()
        pltpu.make_async_copy(d_hbm.at[layer, c], wd.at[i, z, k], ownsem.at[1, i]).start()

    def gather2(i):
        wait_bytes(wgu.at[i, 0, pl.ds(0, LINE - 1), 0, 0], a1recv.at[0, i])
        wait_bytes(wd.at[i, pl.ds(0, LINE - 1), 0, 0, :, pl.ds(0, D // 2)], a1recv.at[1, i])
        for o in range(1, LINE):
            gu, down = quarter(i, (z + o) % LINE)
            for p in range(1, REPS):
                to = {"rep": (rep + p) % REPS}
                pltpu.make_async_remote_copy(gu, gu, a2send.at[0], a2recv.at[0, i], device_id=to).start()
                pltpu.make_async_remote_copy(down, down, a2send.at[1], a2recv.at[1, i], device_id=to).start()

    def gather3(i):
        wait_bytes(wgu.at[pl.ds(0, REPS - 1), 0, pl.ds(0, LINE - 1), 0, 0], a2recv.at[0, i])
        wait_bytes(wd.at[pl.ds(0, REPS - 1), pl.ds(0, LINE - 1), 0, 0, :, pl.ds(0, D // 2)], a2recv.at[1, i])
        wait_bytes(wgu.at[i, :, 0, 0], ownsem.at[0, i])
        wait_bytes(wd.at[i, 0, 0], ownsem.at[1, i])
        gu, down = wgu.at[i, :, :, k], wd.at[i, :, k]
        to = {"dp": z * CORES + other}
        pltpu.make_async_remote_copy(gu, gu, a3send.at[0], a3recv.at[0, i], device_id=to).start()
        pltpu.make_async_remote_copy(down, down, a3send.at[1], a3recv.at[1, i], device_id=to).start()

    def arrived(i):
        wait_bytes(wgu.at[i, :, :, 0], a3recv.at[0, i])
        wait_bytes(wd.at[i, :, 0], a3recv.at[1, i])

    def gather_on(i, t):
        pl.when((t == 1) & (i + AHEAD < ALL))(lambda: gather1(i + AHEAD))
        pl.when((t == 1) & (i + 2 < ALL))(lambda: gather2(i + 2))
        pl.when((t == 2) & (i + 1 < ALL))(lambda: gather3(i + 1))

    pl.loop(0, AHEAD)(gather1)
    acc[...] = jnp.zeros_like(acc)

    @pl.loop(0, TILES)
    def _(t):
        fetch(x_hbm, xb, xsem, t).wait()
        wide = xb[tokens(t)].astype(F32)
        abuf[tokens(t)] = (wide * norm_scale(wide)).astype(BF16)

    gather2(0)
    gather2(1)
    gather3(0)

    def weights(i):
        gu = wgu[i]
        return gu[0].reshape(D, CHUNK), gu[1].reshape(D, CHUNK), wd[i].reshape(CHUNK, D)

    @pl.loop(0, CHUNKS)
    def _(c):
        arrived(c)

        @pl.loop(0, TILES)
        def _(t):
            gather_on(c, t)
            wg, wu, down = weights(c)
            a = abuf[tokens(t)]
            gate, up = dot(a, wg), dot(a, wu)
            hidden = (gate * jax.nn.sigmoid(gate) * up).astype(BF16)
            acc[tokens(t)] += dot(hidden, down)

    @pl.loop(0, TILES)
    def _(t):
        h = xb[tokens(t)] + acc[tokens(t)].astype(BF16)
        xb[tokens(t)] = h
        wide = h.astype(F32)
        abuf[tokens(t)] = (wide * norm_scale(wide)).astype(BF16)
        acc[tokens(t)] = jnp.zeros((TILE, D), F32)
        fetch(dy_hbm, dyb, dysem, t).wait()

    def backward(i, t, s, with_input):
        wg, wu, down = weights(i)
        a, by_y = abuf[tokens(t)], dyb[tokens(t)]
        gate, up = dot(a, wg), dot(a, wu)
        by_hidden = dot(by_y, down, 1, 1).astype(BF16).astype(F32)
        sig = jax.nn.sigmoid(gate)
        silu = gate * sig
        hidden = (silu * up).astype(BF16)
        by_up = (by_hidden * silu).astype(BF16)
        by_gate = (by_hidden * up * (sig + silu * (1.0 - sig))).astype(BF16)

        def add(ref, value):
            ref[...] = jnp.where(t == 0, 0.0, ref[...]) + value.reshape(ref.shape)

        add(gd.at[s], dot(hidden, by_y, 0, 0))
        add(gg.at[s, 0], dot(a, by_gate, 0, 0))
        add(gg.at[s, 1], dot(a, by_up, 0, 0))
        if with_input:
            acc[tokens(t)] += dot(by_gate, wg, 1, 1) + dot(by_up, wu, 1, 1)

    def partner_copies(q):
        to, s = {"dp": z * CORES + other}, q % 2
        return (
            pltpu.make_async_remote_copy(s1gu, r1gu.at[s], c1send.at[0], c1recv.at[0, s], device_id=to),
            pltpu.make_async_remote_copy(s1d, r1d.at[s], c1send.at[1], c1recv.at[1, s], device_id=to),
        )

    def scatter1(q):
        s1gu[...] = gg[q % 2, :, :, other].astype(BF16)
        s1d[...] = gd[q % 2, :, other].astype(BF16)
        for copy in partner_copies(q):
            copy.start()

    mate, side = z + 1 - 2 * (z % 2), z // 2
    across = (LINE // 2) * (1 - side)
    middle = (z + 1) // 2 % 2 == 1

    def mate_copies(q):
        to, s, r = {"dp": mate * CORES + k}, q % 2, q % SLOTS
        return (
            pltpu.make_async_remote_copy(s2d.at[s], r2d.at[r], c2send.at[0, s], c2recv.at[0, r], device_id=to),
            pltpu.make_async_remote_copy(s2gu.at[s], r2gu.at[r], c2send.at[1, s], c2recv.at[1, r], device_id=to),
        )

    def end_copies(q):
        to, s, r = {"dp": mate * CORES + k}, q % 2, q % SLOTS
        return (
            pltpu.make_async_remote_copy(sod.at[s], rod.at[r], cosend.at[0, s], corecv.at[0, r], device_id=to),
            pltpu.make_async_remote_copy(sogu.at[s], rogu.at[r], cosend.at[1, s], corecv.at[1, r], device_id=to),
        )

    def scatter2(q):
        s = q % 2
        for copy in partner_copies(q):
            copy.wait()

        @pl.when(q >= 2)
        def _():
            for copy in mate_copies(q):
                copy.wait_send()

            @pl.when(jnp.logical_not(middle))
            def _():
                for copy in end_copies(q):
                    copy.wait_send()

        pl.when(q >= SLOTS)(lambda: pl.semaphore_wait(mate_free, 1))
        two = pl.ds(across, LINE // 2)

        @pl.when(jnp.logical_not(middle))
        def _():
            sod[s] = (gd[s, two, k] + r1d[s, two].astype(F32)).astype(BF16)
            for g in range(2):
                sogu[s, g] = (gg[s, g, two, k] + r1gu[s, g, two].astype(F32)).astype(BF16)
            for copy in end_copies(q):
                copy.start()

        @pl.when(middle)
        def _():
            sumod[...] = gd[s, two, k] + r1d[s, two].astype(F32)
            for g in range(2):
                sumogu[g] = gg[s, g, two, k] + r1gu[s, g, two].astype(F32)

        s2d[s] = (gd[s, mate, k] + r1d[s, mate].astype(F32)).astype(BF16)
        for g in range(2):
            s2gu[s, g] = (gg[s, g, mate, k] + r1gu[s, g, mate].astype(F32)).astype(BF16)
        for copy in mate_copies(q):
            copy.start()
        sum_d[s] = gd[s, z, k] + r1d[s, z].astype(F32)
        for g in range(2):
            sum_gu[s, g] = gg[s, g, z, k] + r1gu[s, g, z].astype(F32)

    def across_copies(q, array):
        s, r = q % 2, q % SLOTS
        to = [{"dp": (across + u) * CORES + k} for u in range(2)]
        if array == 0:
            return [pltpu.make_async_remote_copy(s3d.at[s, u], r3d.at[r], c3send.at[0, s, u], c3recv.at[0, r], device_id=to[u]) for u in range(2)]
        return [pltpu.make_async_remote_copy(s3gu.at[s, u], r3gu.at[r], c3send.at[1, s, u], c3recv.at[1, r], device_id=to[u]) for u in range(2)]

    def scatter3(q):
        @pl.when(middle)
        def _():
            s, r = q % 2, q % SLOTS

            @pl.when(q >= 2)
            def _():
                for copy in across_copies(q, 0) + across_copies(q, 1):
                    copy.wait_send()

            @pl.when(q >= SLOTS)
            def _():
                for u in range(2):
                    pl.semaphore_wait(across_free.at[u], 1)

            wait_bytes(rod.at[r], corecv.at[0, r])
            for u in range(2):
                s3d[s, u] = (sumod[u] + rod[r, u].astype(F32)).astype(BF16)
            for copy in across_copies(q, 0):
                copy.start()
            wait_bytes(rogu.at[r], corecv.at[1, r])
            for u in range(2):
                for g in range(2):
                    s3gu[s, u, g] = (sumogu[g, u] + rogu[r, g, u].astype(F32)).astype(BF16)
            for copy in across_copies(q, 1):
                copy.start()

    def scatter4(q):
        s, r = q % 2, q % SLOTS
        wait_bytes(r2d.at[r], c2recv.at[0, r])
        wait_bytes(r2gu.at[r], c2recv.at[1, r])
        wait_bytes(r3d.at[r], c3recv.at[0, r])
        wait_bytes(r3gu.at[r], c3recv.at[1, r])
        total_gu = sum_gu[s] + r2gu[r].astype(F32) + r3gu[r].astype(F32)
        total_d = sum_d[s] + r2d[r].astype(F32) + r3d[r].astype(F32)

        @pl.when(q + SLOTS < ALL)
        def _():
            pl.semaphore_signal(mate_free, 1, device_id={"dp": mate * CORES + k})
            pl.semaphore_signal(across_free.at[z % 2], 1, device_id={"dp": (2 - side) * CORES + k})

        total_gu, total_d = total_gu.astype(BF16), total_d.astype(BF16)
        layer, c = LAYERS - 1 - q // CHUNKS, q % CHUNKS
        for g in range(2):
            ggu_out[layer, g, :, pl.ds(pl.multiple_of(c * CHUNK, CHUNK), CHUNK)] = total_gu[g]
        gd_out[layer, c] = total_d
        wide_gu, wide_d = total_gu.astype(F32), total_d.astype(F32)
        squares = (wide_gu * wide_gu).reshape(2, ROWS // 8, 8, CHUNK).sum((0, 1))
        squares_d = (wide_d * wide_d).reshape(LOCAL // 8, 8, D).sum(0)
        ssb[0] += sum(squares[:, n : n + 128] for n in range(0, CHUNK, 128)) + sum(squares_d[:, n : n + 128] for n in range(0, D, 128))

    ssb[0] = jnp.zeros((8, 128), F32)

    def layer_backward(base, q0, with_input, weights_come):
        @pl.loop(0, CHUNKS)
        def _(c):
            i, q = base + c, q0 + c
            if weights_come:
                arrived(i)

            @pl.loop(0, TILES)
            def _(t):
                if weights_come:
                    gather_on(i, t)
                pl.when((t == 0) & (q >= 3))(lambda: scatter4(q - 3))
                pl.when((t == 1) & (q >= 2))(lambda: scatter3(q - 2))
                pl.when((t == 1) & (q >= 1))(lambda: scatter2(q - 1))
                backward(i, t, q % 2, with_input)

            scatter1(q)

    layer_backward(CHUNKS, 0, True, True)

    @pl.loop(0, TILES)
    def _(t):
        wide = xb[tokens(t)].astype(F32)
        by_a = acc[tokens(t)].astype(BF16).astype(F32)
        scale = norm_scale(wide)
        inner = jnp.mean(wide * by_a, -1, keepdims=True)
        by_h = by_a * scale - wide * (scale * scale * scale * inner)
        dyb[tokens(t)] = dyb[tokens(t)] + by_h.astype(BF16)
        fetch(x_hbm, xb, xsem, t).start()

    @pl.loop(0, TILES)
    def _(t):
        fetch(x_hbm, xb, xsem, t).wait()
        wide = xb[tokens(t)].astype(F32)
        abuf[tokens(t)] = (wide * norm_scale(wide)).astype(BF16)

    layer_backward(0, CHUNKS, False, False)
    scatter4(ALL - 3)
    scatter3(ALL - 2)
    scatter2(ALL - 1)
    scatter4(ALL - 2)
    scatter3(ALL - 1)
    scatter4(ALL - 1)

    def square_copy(o):
        return pltpu.make_async_remote_copy(ssb.at[0], ssb.at[o], sssend.at[o - 1], ssrecv.at[o - 1], device_id={"dp": (me + o) % GROUP})

    for o in range(1, GROUP):
        square_copy(o).start()
    for o in range(1, GROUP):
        square_copy(o).wait()
    ss_out[...] = sum(ssb[o] for o in range(GROUP))

    for q in (ALL - 2, ALL - 1):
        for copy in mate_copies(q):
            copy.wait_send()

        @pl.when(middle)
        def _(q=q):
            for copy in across_copies(q, 0) + across_copies(q, 1):
                copy.wait_send()

        @pl.when(jnp.logical_not(middle))
        def _(q=q):
            for copy in end_copies(q):
                copy.wait_send()
    wait_bytes(wgu.at[:, 0, pl.ds(0, LINE - 1), 0, 0], a1send.at[0])
    wait_bytes(wd.at[:, pl.ds(0, LINE - 1), 0, 0, :, pl.ds(0, D // 2)], a1send.at[1])
    sent = ALL * (REPS - 1) * (LINE - 1)
    wait_bytes(abuf.at[pl.ds(0, sent * HALF * CHUNK // D)], a2send.at[0])
    wait_bytes(abuf.at[pl.ds(0, sent * LOCAL // 4)], a2send.at[1])
    wait_bytes(wgu.at[:, :, :, 0], a3send.at[0])
    wait_bytes(wd.at[:, :, 0], a3send.at[1])


def gradients(x, dy, gu, down):
    vm, dma = pltpu.VMEM, pltpu.SemaphoreType.DMA
    flops = 17 * 2 * TOKENS * D * FF
    return pl.pallas_call(
        kernel,
        out_shape=(
            jax.ShapeDtypeStruct((LAYERS, 2, ROWS, FF), BF16),
            jax.ShapeDtypeStruct((LAYERS, CHUNKS, LOCAL, D), BF16),
            jax.ShapeDtypeStruct((8, 128), F32),
        ),
        in_specs=[pl.BlockSpec(memory_space=pl.ANY)] * 4,
        out_specs=(pl.BlockSpec(memory_space=pltpu.VMEM),) * 3,
        scratch_shapes=[
            vm((TOKENS, D), BF16), vm((TOKENS, D), BF16), vm((TOKENS, D), BF16), vm((TOKENS, D), F32),
            vm((ALL, 2, LINE, CORES, 2, HALF, CHUNK), BF16), vm((ALL, LINE, CORES, 2, LOCAL // 2, D), BF16),
            vm((2, 2, LINE, CORES, ROWS, CHUNK), F32), vm((2, LINE, CORES, LOCAL, D), F32),
            vm((2, LINE, ROWS, CHUNK), BF16), vm((LINE, LOCAL, D), BF16),
            vm((2, 2, LINE, ROWS, CHUNK), BF16), vm((2, LINE, LOCAL, D), BF16),
            vm((2, 2, ROWS, CHUNK), F32), vm((2, LOCAL, D), F32),
            vm((2, 2, ROWS, CHUNK), BF16), vm((2, LOCAL, D), BF16), vm((SLOTS, 2, ROWS, CHUNK), BF16), vm((SLOTS, LOCAL, D), BF16),
            vm((2, 2, 2, ROWS, CHUNK), BF16), vm((2, 2, LOCAL, D), BF16), vm((SLOTS, 2, 2, ROWS, CHUNK), BF16), vm((SLOTS, 2, LOCAL, D), BF16),
            vm((2, 2, ROWS, CHUNK), F32), vm((2, LOCAL, D), F32),
            vm((2, 2, 2, ROWS, CHUNK), BF16), vm((2, 2, LOCAL, D), BF16), vm((SLOTS, 2, ROWS, CHUNK), BF16), vm((SLOTS, LOCAL, D), BF16),
            vm((GROUP, 8, 128), F32),
            dma((TILES,)), dma((TILES,)), dma((2, ALL)), dma((2,)), dma((2, ALL)), dma((2,)), dma((2, ALL)), dma((2,)), dma((2, ALL)),
            dma((2,)), dma((2, 2)), dma((2, 2)), dma((2, SLOTS)), dma((2, 2)), dma((2, SLOTS)), dma((2, 2, 2)), dma((2, SLOTS)),
            pltpu.SemaphoreType.REGULAR, pltpu.SemaphoreType.REGULAR((2,)), dma((GROUP - 1,)), dma((GROUP - 1,)),
        ],
        compiler_params=pltpu.CompilerParams(collective_id=0, has_side_effects=True, vmem_limit_bytes=67043328),
        cost_estimate=pl.CostEstimate(flops=flops, bytes_accessed=2 * TOKENS * D * 2, transcendentals=0),
    )(x, dy, gu, down)


def solution(mesh):
    def step(x, dy, w_gate, w_up, w_down, m_gate, m_up, m_down, v_gate, v_up, v_down):
        own = lax.optimization_barrier(jnp.asarray(ORDER))
        order = (lax.broadcasted_iota(jnp.int32, (FF, FF), 0) == own[None, :]).astype(BF16)
        gu = jnp.stack([w_gate, w_up], 1)
        placed = jnp.dot(gu.reshape(-1, FF), order, preferred_element_type=F32).astype(BF16)
        ggu, gd, squares = gradients(
            x, dy, placed.reshape(LAYERS, 2, 2, HALF, FF), w_down.reshape(LAYERS, CHUNKS, 2, LOCAL // 2, D)
        )
        ggu = lax.dot_general(ggu.reshape(-1, FF), order, (((1,), (1,)), ((), ())), preferred_element_type=F32)
        ggu = ggu.astype(BF16).astype(F32).reshape(LAYERS, 2, ROWS, FF)
        g = [ggu[:, 0], ggu[:, 1], gd.reshape(w_down.shape).astype(F32)]
        count = GROUP * sum(one.size for one in g)
        factor = jnp.minimum(1.0, 0.5 * lax.rsqrt(jnp.sum(squares) / count + 1e-30))
        new = [
            adamw(w.astype(F32), m, v, one * factor)
            for w, m, v, one in zip((w_gate, w_up, w_down), (m_gate, m_up, m_down), (v_gate, v_up, v_down), g, strict=True)
        ]
        return tuple(one[which] for which in range(3) for one in new)

    states, cut = P(("rep", "dp"), None, None), P(None, "dp", None)
    return jax.shard_map(
        step,
        mesh=mesh,
        in_specs=(states, states) + (cut,) * 9,
        out_specs=(P("rep", "dp", None),) * 9,
        check_vma=False,
    )
```

```python
import functools

import jax
import jax.numpy as jnp
from jax import lax
from jax.experimental import pallas as pl
from jax.experimental.pallas import tpu as pltpu
from jax.sharding import PartitionSpec as P

LAYERS, TOKENS, D, FF = 2, 4096, 768, 1792
REPS, LINE, CORES = 4, 4, 2
GROUP = LINE * CORES
CHUNK = 256
CHUNKS = FF // CHUNK
LOCAL = CHUNK // GROUP
ROWS = D // GROUP
HALF = ROWS // 2
TILE = 1024
TILES = TOKENS // TILE
AHEAD = 4
SLOTS = 3
ALL = LAYERS * CHUNKS
F32, BF16 = jnp.float32, jnp.bfloat16


def adamw(w, m, v, g):
    m = 0.9 * m + 0.1 * g
    v = 0.95 * v + 0.05 * g * g
    step = m * lax.rsqrt(v + 1e-8) + 0.1 * w
    return (w - 0.02 * step).astype(BF16), m, v


def dot(a, b, ca=1, cb=0):
    return lax.dot_general(a, b, (((ca,), (cb,)), ((), ())), preferred_element_type=F32)


def norm_scale(wide):
    return lax.rsqrt(jnp.mean(wide * wide, -1, keepdims=True) + 1e-6)


def kernel(
    x_hbm, dy_hbm, gate_hbm, up_hbm, d_hbm, gate_out, up_out, gd_out, ss_out,
    placed, abuf, xb, dyb, acc, wgu, wd, gg, gd,
    s1gu, s1d, r1gu, r1d, sum_gu, sum_d, s2gu, s2d, r2gu, r2d, sogu, sod, rogu, rod, sumogu, sumod, s3gu, s3d, r3gu, r3d, ssb,
    xsem, dysem, gusem, ownsem, a1send, a1recv, a2send, a2recv, a3send, a3recv,
    c1send, c1recv, c2send, c2recv, cosend, corecv, c3send, c3recv, mate_free, across_free, sssend, ssrecv,
):
    rep, me = lax.axis_index("rep"), lax.axis_index("dp")
    z, k = me // CORES, me % CORES
    other = 1 - k
    rg, rh = rep // 2, rep % 2

    barrier = pltpu.get_barrier_semaphore()
    for o in range(1, GROUP):
        pl.semaphore_signal(barrier, 1, device_id={"dp": (me + o) % GROUP})
    for o in range(1, REPS):
        pl.semaphore_signal(barrier, 1, device_id={"rep": (rep + o) % REPS})

    def tokens(t):
        return pl.ds(pl.multiple_of(t * TILE, TILE), TILE)

    def fetch(hbm, vmem, sem, t):
        return pltpu.make_async_copy(hbm.at[0, tokens(t)], vmem.at[tokens(t)], sem.at[t])

    raw = [pltpu.make_async_copy(hbm, placed.at[:, g], gusem.at[0, g]) for g, hbm in enumerate((gate_hbm, up_hbm))]
    for copy in raw:
        copy.start()
    for t in range(TILES):
        fetch(x_hbm, xb, xsem, t).start()
        fetch(dy_hbm, dyb, dysem, t).start()

    def chosen(c):
        place = lax.broadcasted_iota(jnp.int32, (1, CHUNK), 1)
        column = place // LOCAL * (FF // GROUP) + place % LOCAL + c * LOCAL
        return jnp.where(lax.broadcasted_iota(jnp.int32, (FF, CHUNK), 0) == column, 1.0, 0.0).astype(BF16)

    def place(c):
        columns = dot(placed[...].reshape(LAYERS * 2 * ROWS, FF), chosen(c)).astype(BF16).reshape(LAYERS, 2, 2, HALF, CHUNK)
        for layer in range(LAYERS):
            for g in range(2):
                wgu[layer * CHUNKS + c, g, z, k] = columns[layer, g]

    for copy in raw:
        copy.wait()
    place(0)
    pl.semaphore_wait(barrier, GROUP - 1 + REPS - 1)

    def wait_bytes(ref, sem):
        pltpu.make_async_copy(ref, ref, sem).wait()

    d_half = pl.ds(pl.multiple_of(rh * (D // 2), D // 2), D // 2)

    def quarter(i, line):
        return wgu.at[i, rg, line, k, rh], wd.at[i, line, k, rg, :, d_half]

    def gather1(i):
        layer, c = i // CHUNKS, i % CHUNKS
        gu_to, d_to = quarter(i, z)
        gu, down = gu_to, d_hbm.at[layer, c, rg, :, d_half]
        for o in range(1, LINE):
            to = {"dp": (z + o) % LINE * CORES + k}
            pltpu.make_async_remote_copy(gu, gu_to, a1send.at[0], a1recv.at[0, i], device_id=to).start()
            pltpu.make_async_remote_copy(down, d_to, a1send.at[1], a1recv.at[1, i], device_id=to).start()
        pltpu.make_async_copy(d_hbm.at[layer, c], wd.at[i, z, k], ownsem.at[i]).start()

    def gather2(i):
        wait_bytes(wgu.at[i, 0, pl.ds(0, LINE - 1), 0, 0], a1recv.at[0, i])
        wait_bytes(wd.at[i, pl.ds(0, LINE - 1), 0, 0, :, pl.ds(0, D // 2)], a1recv.at[1, i])
        for o in range(1, LINE):
            gu, down = quarter(i, (z + o) % LINE)
            for p in range(1, REPS):
                to = {"rep": (rep + p) % REPS}
                pltpu.make_async_remote_copy(gu, gu, a2send.at[0], a2recv.at[0, i], device_id=to).start()
                pltpu.make_async_remote_copy(down, down, a2send.at[1], a2recv.at[1, i], device_id=to).start()

    def gather3(i):
        wait_bytes(wgu.at[pl.ds(0, REPS - 1), 0, pl.ds(0, LINE - 1), 0, 0], a2recv.at[0, i])
        wait_bytes(wd.at[pl.ds(0, REPS - 1), pl.ds(0, LINE - 1), 0, 0, :, pl.ds(0, D // 2)], a2recv.at[1, i])
        wait_bytes(wd.at[i, 0, 0], ownsem.at[i])
        gu, down = wgu.at[i, :, :, k], wd.at[i, :, k]
        to = {"dp": z * CORES + other}
        pltpu.make_async_remote_copy(gu, gu, a3send.at[0], a3recv.at[0, i], device_id=to).start()
        pltpu.make_async_remote_copy(down, down, a3send.at[1], a3recv.at[1, i], device_id=to).start()

    def arrived(i):
        wait_bytes(wgu.at[i, :, :, 0], a3recv.at[0, i])
        wait_bytes(wd.at[i, :, 0], a3recv.at[1, i])

    def gather_on(i, t):
        pl.when((t == 0) & (i == 0))(lambda: gather2(2))
        pl.when((t == 1) & (i + AHEAD < ALL))(lambda: gather1(i + AHEAD))
        pl.when((t == 2) & (i + 1 < ALL))(lambda: gather3(i + 1))
        pl.when((t == 3) & (i + 3 < ALL))(lambda: gather2(i + 3))

    gather1(0)

    @pl.loop(1, AHEAD)
    def _(c):
        place(c)
        gather1(c)

    def norm_tile(t):
        fetch(x_hbm, xb, xsem, t).wait()
        wide = xb[tokens(t)].astype(F32)
        abuf[tokens(t)] = (wide * norm_scale(wide)).astype(BF16)

    pl.loop(0, TILES // 2)(norm_tile)
    gather2(0)
    pl.loop(AHEAD, CHUNKS)(place)
    acc[...] = jnp.zeros_like(acc)
    gather2(1)
    pl.loop(TILES // 2, TILES)(norm_tile)
    gather3(0)

    def weights(i):
        gu = wgu[i]
        return gu[0].reshape(D, CHUNK), gu[1].reshape(D, CHUNK), wd[i].reshape(CHUNK, D)

    @pl.loop(0, CHUNKS)
    def _(c):
        arrived(c)

        @pl.loop(0, TILES // 2)
        def _(t):
            gather_on(c, 2 * t)
            gather_on(c, 2 * t + 1)
            there = pl.ds(pl.multiple_of(t * 2 * TILE, 2 * TILE), 2 * TILE)
            wg, wu, down = weights(c)
            a = abuf[there]
            gate, up = dot(a, wg), dot(a, wu)
            hidden = (gate * jax.nn.sigmoid(gate) * up).astype(BF16)
            acc[there] += dot(hidden, down)

    @pl.loop(0, TILES)
    def _(t):
        h = xb[tokens(t)] + acc[tokens(t)].astype(BF16)
        xb[tokens(t)] = h
        wide = h.astype(F32)
        abuf[tokens(t)] = (wide * norm_scale(wide)).astype(BF16)
        acc[tokens(t)] = jnp.zeros((TILE, D), F32)
        fetch(dy_hbm, dyb, dysem, t).wait()

    def backward(i, t, s, with_input):
        wg, wu, down = weights(i)
        a, by_y = abuf[tokens(t)], dyb[tokens(t)]
        gate, up = dot(a, wg), dot(a, wu)
        by_hidden = dot(by_y, down, 1, 1).astype(BF16).astype(F32)
        sig = jax.nn.sigmoid(gate)
        silu = gate * sig
        hidden = (silu * up).astype(BF16)
        by_up = (by_hidden * silu).astype(BF16)
        by_gate = (by_hidden * up * (sig + silu * (1.0 - sig))).astype(BF16)

        def add(ref, value):
            ref[...] = jnp.where(t == 0, 0.0, ref[...]) + value.reshape(ref.shape)

        add(gd.at[s], dot(hidden, by_y, 0, 0))
        add(gg.at[s, 0], dot(a, by_gate, 0, 0))
        add(gg.at[s, 1], dot(a, by_up, 0, 0))
        if with_input:
            acc[tokens(t)] += dot(by_gate, wg, 1, 1) + dot(by_up, wu, 1, 1)

    def partner_copies(q):
        to, s = {"dp": z * CORES + other}, q % 2
        return (
            pltpu.make_async_remote_copy(s1gu, r1gu.at[s], c1send.at[0], c1recv.at[0, s], device_id=to),
            pltpu.make_async_remote_copy(s1d, r1d.at[s], c1send.at[1], c1recv.at[1, s], device_id=to),
        )

    def scatter1(q):
        s1gu[...] = gg[q % 2, :, :, other].astype(BF16)
        s1d[...] = gd[q % 2, :, other].astype(BF16)
        for copy in partner_copies(q):
            copy.start()

    mate, side = z + 1 - 2 * (z % 2), z // 2
    across = (LINE // 2) * (1 - side)
    middle = (z + 1) // 2 % 2 == 1

    def mate_copies(q):
        to, s, r = {"dp": mate * CORES + k}, q % 2, q % SLOTS
        return (
            pltpu.make_async_remote_copy(s2d.at[s], r2d.at[r], c2send.at[0, s], c2recv.at[0, r], device_id=to),
            pltpu.make_async_remote_copy(s2gu.at[s], r2gu.at[r], c2send.at[1, s], c2recv.at[1, r], device_id=to),
        )

    def end_copies(q):
        to, s, r = {"dp": mate * CORES + k}, q % 2, q % SLOTS
        return (
            pltpu.make_async_remote_copy(sod.at[s], rod.at[r], cosend.at[0, s], corecv.at[0, r], device_id=to),
            pltpu.make_async_remote_copy(sogu.at[s], rogu.at[r], cosend.at[1, s], corecv.at[1, r], device_id=to),
        )

    def scatter2(q):
        s = q % 2
        for copy in partner_copies(q):
            copy.wait()

        @pl.when(q >= 2)
        def _():
            for copy in mate_copies(q):
                copy.wait_send()

            @pl.when(jnp.logical_not(middle))
            def _():
                for copy in end_copies(q):
                    copy.wait_send()

        pl.when(q >= SLOTS)(lambda: pl.semaphore_wait(mate_free, 1))
        two = pl.ds(across, LINE // 2)

        @pl.when(jnp.logical_not(middle))
        def _():
            sod[s] = (gd[s, two, k] + r1d[s, two].astype(F32)).astype(BF16)
            for g in range(2):
                sogu[s, g] = (gg[s, g, two, k] + r1gu[s, g, two].astype(F32)).astype(BF16)
            for copy in end_copies(q):
                copy.start()

        @pl.when(middle)
        def _():
            sumod[...] = gd[s, two, k] + r1d[s, two].astype(F32)
            for g in range(2):
                sumogu[g] = gg[s, g, two, k] + r1gu[s, g, two].astype(F32)

        s2d[s] = (gd[s, mate, k] + r1d[s, mate].astype(F32)).astype(BF16)
        for g in range(2):
            s2gu[s, g] = (gg[s, g, mate, k] + r1gu[s, g, mate].astype(F32)).astype(BF16)
        for copy in mate_copies(q):
            copy.start()
        sum_d[s] = gd[s, z, k] + r1d[s, z].astype(F32)
        for g in range(2):
            sum_gu[s, g] = gg[s, g, z, k] + r1gu[s, g, z].astype(F32)

    def across_copies(q, array):
        s, r = q % 2, q % SLOTS
        to = [{"dp": (across + u) * CORES + k} for u in range(2)]
        if array == 0:
            return [pltpu.make_async_remote_copy(s3d.at[s, u], r3d.at[r], c3send.at[0, s, u], c3recv.at[0, r], device_id=to[u]) for u in range(2)]
        return [pltpu.make_async_remote_copy(s3gu.at[s, u], r3gu.at[r], c3send.at[1, s, u], c3recv.at[1, r], device_id=to[u]) for u in range(2)]

    def scatter3(q):
        @pl.when(middle)
        def _():
            s, r = q % 2, q % SLOTS

            @pl.when(q >= 2)
            def _():
                for copy in across_copies(q, 0) + across_copies(q, 1):
                    copy.wait_send()

            @pl.when(q >= SLOTS)
            def _():
                for u in range(2):
                    pl.semaphore_wait(across_free.at[u], 1)

            wait_bytes(rod.at[r], corecv.at[0, r])
            for u in range(2):
                s3d[s, u] = (sumod[u] + rod[r, u].astype(F32)).astype(BF16)
            for copy in across_copies(q, 0):
                copy.start()
            wait_bytes(rogu.at[r], corecv.at[1, r])
            for u in range(2):
                for g in range(2):
                    s3gu[s, u, g] = (sumogu[g, u] + rogu[r, g, u].astype(F32)).astype(BF16)
            for copy in across_copies(q, 1):
                copy.start()

    def scatter4(q):
        s, r = q % 2, q % SLOTS
        wait_bytes(r2d.at[r], c2recv.at[0, r])
        wait_bytes(r2gu.at[r], c2recv.at[1, r])
        wait_bytes(r3d.at[r], c3recv.at[0, r])
        wait_bytes(r3gu.at[r], c3recv.at[1, r])
        total_gu = sum_gu[s] + r2gu[r].astype(F32) + r3gu[r].astype(F32)
        total_d = sum_d[s] + r2d[r].astype(F32) + r3d[r].astype(F32)

        @pl.when(q + SLOTS < ALL)
        def _():
            pl.semaphore_signal(mate_free, 1, device_id={"dp": mate * CORES + k})
            pl.semaphore_signal(across_free.at[z % 2], 1, device_id={"dp": (2 - side) * CORES + k})

        total_gu, total_d = total_gu.astype(BF16), total_d.astype(BF16)
        layer, c = LAYERS - 1 - q // CHUNKS, q % CHUNKS
        for g in range(2):
            placed[layer, g, :, pl.ds(pl.multiple_of(c * CHUNK, CHUNK), CHUNK)] = total_gu[g]
        gd_out[layer, c] = total_d
        wide_gu, wide_d = total_gu.astype(F32), total_d.astype(F32)
        squares = (wide_gu * wide_gu).reshape(2, ROWS // 8, 8, CHUNK).sum((0, 1))
        squares_d = (wide_d * wide_d).reshape(LOCAL // 8, 8, D).sum(0)
        ssb[0] += sum(squares[:, n : n + 128] for n in range(0, CHUNK, 128)) + sum(squares_d[:, n : n + 128] for n in range(0, D, 128))

    def block(layer, n):
        return acc.at[pl.ds((layer * 3 + n // 3) * 2 * ROWS, 2 * ROWS), n % 3 * CHUNK : (n % 3 + 1) * CHUNK]

    def put_back(layer, c):
        columns = placed[layer, :, :, pl.ds(pl.multiple_of(c * CHUNK, CHUNK), CHUNK)].reshape(2 * ROWS, CHUNK)
        to = chosen(c)
        for n in range(CHUNKS):
            there = block(layer, n)
            there[...] = jnp.where(c == 0, 0.0, there[...]) + dot(columns, to[n * CHUNK : (n + 1) * CHUNK], 1, 1)

    def out_copies(layer):
        return [pltpu.make_async_copy(placed.at[layer, g], out.at[layer], gusem.at[layer, g]) for g, out in enumerate((gate_out, up_out))]

    def put_out(layer):
        for n in range(CHUNKS):
            placed[layer, :, :, n * CHUNK : (n + 1) * CHUNK] = block(layer, n)[...].astype(BF16).reshape(2, ROWS, CHUNK)
        for copy in out_copies(layer):
            copy.start()

    ssb[0] = jnp.zeros((8, 128), F32)

    def layer_backward(base, q0, with_input, weights_come):
        @pl.loop(0, CHUNKS)
        def _(c):
            i, q = base + c, q0 + c
            if weights_come:
                arrived(i)

            @pl.loop(0, TILES)
            def _(t):
                if weights_come:
                    gather_on(i, t)
                pl.when((t == 0) & (q >= 3))(lambda: scatter4(q - 3))
                pl.when((t == 1) & (q >= 2))(lambda: scatter3(q - 2))
                pl.when((t == 1) & (q >= 1))(lambda: scatter2(q - 1))
                backward(i, t, q % 2, with_input)

            scatter1(q)

    layer_backward(CHUNKS, 0, True, True)

    @pl.loop(0, TILES)
    def _(t):
        wide = xb[tokens(t)].astype(F32)
        by_a = acc[tokens(t)].astype(BF16).astype(F32)
        scale = norm_scale(wide)
        inner = jnp.mean(wide * by_a, -1, keepdims=True)
        by_h = by_a * scale - wide * (scale * scale * scale * inner)
        dyb[tokens(t)] = dyb[tokens(t)] + by_h.astype(BF16)
        fetch(x_hbm, xb, xsem, t).start()

    @pl.loop(0, TILES)
    def _(t):
        fetch(x_hbm, xb, xsem, t).wait()
        wide = xb[tokens(t)].astype(F32)
        abuf[tokens(t)] = (wide * norm_scale(wide)).astype(BF16)

    layer_backward(0, CHUNKS, False, False)
    scatter4(ALL - 3)
    scatter3(ALL - 2)
    scatter2(ALL - 1)
    pl.loop(0, CHUNKS)(lambda c: put_back(1, c))
    put_out(1)
    scatter4(ALL - 2)
    scatter3(ALL - 1)
    pl.loop(0, CHUNKS - 1)(lambda c: put_back(0, c))
    scatter4(ALL - 1)

    def square_copy(o):
        return pltpu.make_async_remote_copy(ssb.at[0], ssb.at[o], sssend.at[o - 1], ssrecv.at[o - 1], device_id={"dp": (me + o) % GROUP})

    for o in range(1, GROUP):
        square_copy(o).start()
    put_back(0, CHUNKS - 1)
    put_out(0)
    for o in range(1, GROUP):
        square_copy(o).wait()
    ss_out[0, 0] = jnp.sum(sum(ssb[o] for o in range(GROUP)))

    for layer in range(LAYERS):
        for copy in out_copies(layer):
            copy.wait()

    for q in (ALL - 2, ALL - 1):
        for copy in mate_copies(q):
            copy.wait_send()

        @pl.when(middle)
        def _(q=q):
            for copy in across_copies(q, 0) + across_copies(q, 1):
                copy.wait_send()

        @pl.when(jnp.logical_not(middle))
        def _(q=q):
            for copy in end_copies(q):
                copy.wait_send()
    wait_bytes(wgu.at[:, 0, pl.ds(0, LINE - 1), 0, 0], a1send.at[0])
    wait_bytes(wd.at[:, pl.ds(0, LINE - 1), 0, 0, :, pl.ds(0, D // 2)], a1send.at[1])
    sent = ALL * (REPS - 1) * (LINE - 1)
    wait_bytes(abuf.at[pl.ds(0, sent * HALF * CHUNK // D)], a2send.at[0])
    wait_bytes(abuf.at[pl.ds(0, sent * LOCAL // 4)], a2send.at[1])
    wait_bytes(wgu.at[:, :, :, 0], a3send.at[0])
    wait_bytes(wd.at[:, :, 0], a3send.at[1])


def gradients(x, dy, gate, up, down):
    vm, dma = pltpu.VMEM, pltpu.SemaphoreType.DMA
    flops = 17 * 2 * TOKENS * D * FF
    return pl.pallas_call(
        kernel,
        out_shape=(
            jax.ShapeDtypeStruct((LAYERS, ROWS, FF), BF16),
            jax.ShapeDtypeStruct((LAYERS, ROWS, FF), BF16),
            jax.ShapeDtypeStruct((LAYERS, CHUNKS, LOCAL, D), BF16),
            jax.ShapeDtypeStruct((1, 1), F32),
        ),
        in_specs=[pl.BlockSpec(memory_space=pl.ANY)] * 5,
        out_specs=(pl.BlockSpec(memory_space=pl.ANY),) * 2 + (pl.BlockSpec(memory_space=pltpu.VMEM), pl.BlockSpec(memory_space=pltpu.SMEM)),
        scratch_shapes=[
            vm((LAYERS, 2, ROWS, FF), BF16),
            vm((TOKENS, D), BF16), vm((TOKENS, D), BF16), vm((TOKENS, D), BF16), vm((TOKENS, D), F32),
            vm((ALL, 2, LINE, CORES, 2, HALF, CHUNK), BF16), vm((ALL, LINE, CORES, 2, LOCAL // 2, D), BF16),
            vm((2, 2, LINE, CORES, ROWS, CHUNK), F32), vm((2, LINE, CORES, LOCAL, D), F32),
            vm((2, LINE, ROWS, CHUNK), BF16), vm((LINE, LOCAL, D), BF16),
            vm((2, 2, LINE, ROWS, CHUNK), BF16), vm((2, LINE, LOCAL, D), BF16),
            vm((2, 2, ROWS, CHUNK), F32), vm((2, LOCAL, D), F32),
            vm((2, 2, ROWS, CHUNK), BF16), vm((2, LOCAL, D), BF16), vm((SLOTS, 2, ROWS, CHUNK), BF16), vm((SLOTS, LOCAL, D), BF16),
            vm((2, 2, 2, ROWS, CHUNK), BF16), vm((2, 2, LOCAL, D), BF16), vm((SLOTS, 2, 2, ROWS, CHUNK), BF16), vm((SLOTS, 2, LOCAL, D), BF16),
            vm((2, 2, ROWS, CHUNK), F32), vm((2, LOCAL, D), F32),
            vm((2, 2, 2, ROWS, CHUNK), BF16), vm((2, 2, LOCAL, D), BF16), vm((SLOTS, 2, ROWS, CHUNK), BF16), vm((SLOTS, LOCAL, D), BF16),
            vm((GROUP, 8, 128), F32),
            dma((TILES,)), dma((TILES,)), dma((LAYERS, 2)), dma((ALL,)), dma((2,)), dma((2, ALL)), dma((2,)), dma((2, ALL)), dma((2,)), dma((2, ALL)),
            dma((2,)), dma((2, 2)), dma((2, 2)), dma((2, SLOTS)), dma((2, 2)), dma((2, SLOTS)), dma((2, 2, 2)), dma((2, SLOTS)),
            pltpu.SemaphoreType.REGULAR, pltpu.SemaphoreType.REGULAR((2,)), dma((GROUP - 1,)), dma((GROUP - 1,)),
        ],
        compiler_params=pltpu.CompilerParams(collective_id=0, has_side_effects=True, vmem_limit_bytes=67043328),
        cost_estimate=pl.CostEstimate(flops=flops, bytes_accessed=2 * TOKENS * D * 2, transcendentals=0),
    )(x, dy, gate, up, down)


def solution(mesh):
    def step(x, dy, w_gate, w_up, w_down, m_gate, m_up, m_down, v_gate, v_up, v_down):
        g_gate, g_up, g_down, squares = gradients(x, dy, w_gate, w_up, w_down.reshape(LAYERS, CHUNKS, 2, LOCAL // 2, D))
        g = [g_gate, g_up, g_down.reshape(w_down.shape)]
        count = GROUP * sum(one.size for one in g)
        factor = jnp.minimum(1.0, 0.5 * lax.rsqrt(squares.reshape(()) / count + 1e-30))
        new = [
            adamw(w.astype(F32), m, v, one.astype(F32) * factor)
            for w, m, v, one in zip((w_gate, w_up, w_down), (m_gate, m_up, m_down), (v_gate, v_up, v_down), g, strict=True)
        ]
        return tuple(one[which] for which in range(3) for one in new)

    states, cut = P(("rep", "dp"), None, None), P(None, "dp", None)
    return jax.shard_map(
        step,
        mesh=mesh,
        in_specs=(states, states) + (cut,) * 9,
        out_specs=(P("rep", "dp", None),) * 9,
        check_vma=False,
    )
```
